32 devices in a mesh: blk: 16 (over z, y, core), tp: 2 (over x).
Axes of the slice: x: 2, y: 2, z: 4, core: 2. Of those that a mesh axis runs over, the one named last changes fastest.
Arguments:
- dec_states: bfloat16 [4096, 5120], P('blk', 'tp'), may hold values from -200 to 200
- norm_gain: float32 [5120], replicated, may hold values from 0.1 to 1.9
- query_weight: bfloat16 [5120, 768], P(None, 'tp'), may hold values from -0.078125 to 0.078125
- out_weight: bfloat16 [768, 5120], P('tp'), may hold values from -0.21875 to 0.21875
- enc_keys: bfloat16 [6144, 768], P('blk', 'tp'), may hold values from -1000 to 1000
- enc_values: bfloat16 [6144, 768], P('blk', 'tp'), may hold values from -6 to 6
Outputs:
- attn_out: bfloat16 [4096, 5120], P('blk', 'tp')
The draws below stay inside these ranges and needn't reach their ends.
All inputs are finite; a program needn't handle non-finite values.
Results may differ from the reference program's by a relative error of at most 0.034.
Values may be sent and summed in bfloat16 or wider, within the bound.
A program may use at most 128 MiB of HBM per device.

```python
import math
import jax
import jax.numpy as jnp
from jax import lax

D = 5120
HEAD_DIM = 128
Q_DEV = 256
HEADS = 6
DEC_TOK = 4096
ENC_TOK = 6144


def draw_dec_states(key, part):
    key_base, key_rows, key_cols = jax.random.split(key, 3)
    base = jnp.clip(jax.random.normal(key_base, (DEC_TOK, D), jnp.float32), -6.0, 6.0)
    row_scale = jnp.exp(jax.random.uniform(key_rows, (DEC_TOK, 1), jnp.float32) * jnp.log(10.0))
    ramp = 1.0 + 2.0 * jnp.arange(D, dtype=jnp.float32) / D
    col_scale = jnp.exp(jax.random.uniform(key_cols, (1, D), jnp.float32) * jnp.log(10.0)) * ramp[None, :]
    return (base * row_scale * col_scale / 10.0).astype(jnp.bfloat16)


def draw_enc_keys(key, part):
    key_base = jax.random.fold_in(key, 0)
    base = jnp.clip(jax.random.normal(key_base, (ENC_TOK, HEADS * HEAD_DIM), jnp.float32), -6.0, 6.0)
    return base.astype(jnp.bfloat16)


def shard_levels(key, shape, cuts, low, top_value):
    gain = 1.0
    for dim, parts in cuts:
        draws = jax.random.uniform(jax.random.fold_in(jax.random.fold_in(key, 6), dim), (parts,), jnp.float32, low / len(cuts), top_value / len(cuts))
        gain = gain * jnp.repeat(jnp.exp(draws), shape[dim] // parts).reshape((-1,) + (1,) * (len(shape) - 1 - dim))
    return gain


def noise(rng, extent, width, most, pieces=(), kind=jnp.bfloat16):
    values = jax.random.normal(rng, extent, jnp.float32) * width
    if len(pieces) > 0:
        values = shard_levels(rng, extent, pieces, -0.22, 0.18) * values
    return jnp.clip(values, min=-most, max=most).astype(kind)


def setup_inputs(seed: int = 0) -> dict:
    arg_keys = jax.random.split(jax.random.key(seed), 7)
    dec_states = draw_dec_states(jax.random.fold_in(arg_keys[6], 71), 0)
    norm_gain = jnp.clip(1.0 + 0.18 * jax.random.normal(arg_keys[1], (D,), jnp.float32), 0.1, 1.9)
    query_weight = noise(arg_keys[2], (D, HEADS * HEAD_DIM), D ** -0.5, 0.078125, ((1, 2),))
    out_weight = noise(arg_keys[3], (HEADS * HEAD_DIM, D), (HEADS * HEAD_DIM) ** -0.5, 0.21875, ((0, 2),))
    enc_keys = draw_enc_keys(jax.random.fold_in(arg_keys[6], 71), 0)
    enc_values = noise(arg_keys[5], (ENC_TOK, HEADS * HEAD_DIM), 1.0, 6.0, ((0, 16), (1, 2)))
    return {"dec_states": dec_states, "norm_gain": norm_gain, "query_weight": query_weight, "out_weight": out_weight, "enc_keys": enc_keys, "enc_values": enc_values}


NORM_EPS = 1e-06

def reference(dec_states, norm_gain, query_weight, out_weight, enc_keys, enc_values):
    states = dec_states.astype(jnp.float32)
    mean_sq = lax.optimization_barrier(jnp.mean(states * states, axis=1, keepdims=True))
    normed = (states * lax.rsqrt(mean_sq + NORM_EPS) * norm_gain.astype(jnp.float32)).astype(jnp.bfloat16)
    queries = jnp.dot(normed, query_weight, preferred_element_type=jnp.float32).astype(jnp.bfloat16)
    query_heads = queries.reshape(DEC_TOK // Q_DEV, Q_DEV, HEADS, HEAD_DIM).transpose(2, 0, 1, 3)
    key_heads = enc_keys.reshape(ENC_TOK, HEADS, HEAD_DIM).transpose(1, 0, 2)
    value_heads = enc_values.reshape(ENC_TOK, HEADS, HEAD_DIM).transpose(1, 0, 2)
    score_scale = 1.0 / math.sqrt(HEAD_DIM)

    def one_head(operands):
        query_blocks, key_rows, value_rows = operands

        def one_block(query_rows):
            scores = jnp.dot(query_rows, key_rows.T, preferred_element_type=jnp.float32) * score_scale
            row_peak = lax.optimization_barrier(jnp.max(scores, axis=1, keepdims=True))
            exp_scores = jnp.exp(scores - row_peak)
            row_total = lax.optimization_barrier(jnp.sum(exp_scores, axis=1, keepdims=True))
            mixed = jnp.dot(exp_scores.astype(jnp.bfloat16), value_rows, preferred_element_type=jnp.float32)
            return mixed / row_total
        return lax.map(one_block, query_blocks)
    attended = lax.map(one_head, (query_heads, key_heads, value_heads))
    attended = attended.transpose(1, 2, 0, 3).reshape(DEC_TOK, HEADS * HEAD_DIM).astype(jnp.bfloat16)
    return jnp.dot(attended, out_weight, preferred_element_type=jnp.float32).astype(jnp.bfloat16)
```

```python
import functools
import math

import jax
import jax.numpy as jnp
from jax import lax
from jax.experimental import pallas as pl
from jax.experimental.pallas import tpu as pltpu
from jax.sharding import PartitionSpec as P

HEAD_DIM = 128
NORM_EPS = 1e-06
LANES = 128


def column_tile(width, limit=640):
    best = LANES
    for tile in range(LANES, limit + 1, LANES):
        if width % tile == 0:
            best = tile
    return best


def kernel(
    n_blk,
    n_tp,
    x_hbm,
    gain_ref,
    wq_hbm,
    wo_hbm,
    k_hbm,
    v_hbm,
    out_hbm,
    kbuf,
    vbuf,
    wq,
    wo,
    xbuf,
    xg,
    qsend,
    qrecv,
    own_part,
    sqbuf,
    qbuf,
    attbuf,
    obuf,
    row_max,
    row_sum,
    acc,
    kv_send,
    kv_recv,
    tp_send,
    tp_recv,
    sib_send,
    sib_recv,
    local_sem,
    out_sem,
):
    n_line = n_blk // 4
    b = lax.axis_index("blk")
    t = lax.axis_index("tp")
    core = lax.rem(b, 2)
    side = lax.rem(lax.div(b, 2), 2)
    line = lax.div(b, 4)
    rows = x_hbm.shape[0]
    feat = x_hbm.shape[1]
    width = wq_hbm.shape[1]
    heads = width // HEAD_DIM
    half_feat = feat // 2
    half_width = width // 2

    def index(zz, yy, cc):
        return (zz * 2 + yy) * 2 + cc

    sibling = index(line, side, 1 - core)
    beside = index(line, 1 - side, core)
    peers = [lax.rem(t + off, n_tp) for off in range(1, n_tp)]
    bufs = (kbuf, vbuf)

    def ds(start, size, mult=LANES):
        return pl.ds(pl.multiple_of(start, mult), size)

    loads = [
        pltpu.make_async_copy(k_hbm, kbuf.at[b], local_sem.at[0]),
        pltpu.make_async_copy(v_hbm, vbuf.at[b], local_sem.at[1]),
        pltpu.make_async_copy(x_hbm, xbuf, local_sem.at[2]),
        pltpu.make_async_copy(wq_hbm.at[ds(t * feat, feat)], wq.at[t], local_sem.at[3]),
        pltpu.make_async_copy(wo_hbm.at[:, ds(t * feat, feat)], wo.at[t], local_sem.at[4]),
    ]
    for load in loads:
        load.start()

    barrier = pltpu.get_barrier_semaphore()
    has_left = line > 0
    has_right = line < n_line - 1

    @pl.when(has_left)
    def _():
        pl.semaphore_signal(barrier, inc=1, device_id={"blk": b - 4})

    @pl.when(has_right)
    def _():
        pl.semaphore_signal(barrier, inc=1, device_id={"blk": b + 4})

    pl.semaphore_signal(barrier, inc=1, device_id={"blk": sibling})
    pl.semaphore_signal(barrier, inc=1, device_id={"blk": beside})
    for p in peers:
        pl.semaphore_signal(barrier, inc=1, device_id={"tp": p})

    ends = jnp.where(has_left, 1, 0) + jnp.where(has_right, 1, 0)
    pl.semaphore_wait(barrier, 2 + len(peers) + ends)

    def kv_copy(kv, route, zz, yy, cc, target):
        slot = index(zz, yy, cc)
        return pltpu.make_async_remote_copy(
            src_ref=bufs[kv].at[slot],
            dst_ref=bufs[kv].at[slot],
            send_sem=kv_send.at[kv, route, zz],
            recv_sem=kv_recv.at[kv, slot],
            device_id={"blk": target},
        )

    def right_copy(kv, zz):
        return kv_copy(kv, 0, zz, side, core, b + 4)

    def left_copy(kv, zz):
        return kv_copy(kv, 1, zz, side, core, b - 4)

    def beside_copy(kv, zz):
        return kv_copy(kv, 2, zz, side, core, beside)

    def sib_copy(kv, zz):
        return kv_copy(kv, 3, zz, side, core, sibling)

    def sib_beside_copy(kv, zz):
        return kv_copy(kv, 4, zz, 1 - side, core, sibling)

    def wait_slot(kv, zz, yy, cc):
        kv_copy(kv, 0, zz, yy, cc, sibling).wait_recv()

    def column_event(kv, d):
        if d >= n_line:
            return

        @pl.when(line + d < n_line)
        def _():
            zz = line + d
            wait_slot(kv, zz, side, core)

            @pl.when(has_left)
            def _():
                left_copy(kv, zz).start()

            beside_copy(kv, zz).start()
            sib_copy(kv, zz).start()

        @pl.when(line - d >= 0)
        def _():
            zz = line - d
            wait_slot(kv, zz, side, core)

            @pl.when(has_right)
            def _():
                right_copy(kv, zz).start()

            beside_copy(kv, zz).start()
            sib_copy(kv, zz).start()

    def nearest(k):
        short = jnp.minimum(line, n_line - 1 - line)
        swing = line + (k + 1) // 2 if k % 2 == 1 else line - k // 2
        tail = jnp.where(line < n_line - 1 - line, k, n_line - 1 - k)
        return jnp.where(k <= 2 * short, swing, tail)

    def beside_event(k):
        zz = nearest(k)
        for kv in (0, 1):
            wait_slot(kv, zz, 1 - side, core)
            sib_beside_copy(kv, zz).start()

    def wq_copy(i, p):
        return pltpu.make_async_remote_copy(
            src_ref=wq_hbm.at[ds(p * feat + core * half_feat, half_feat)],
            dst_ref=wq.at[t, ds(core * half_feat, half_feat)],
            send_sem=tp_send.at[0, i],
            recv_sem=tp_recv.at[0, t],
            device_id={"tp": p},
        )

    def wq_landed(p):
        return pltpu.make_async_remote_copy(
            src_ref=wq.at[p, ds(core * half_feat, half_feat)],
            dst_ref=wq.at[p, ds(core * half_feat, half_feat)],
            send_sem=tp_send.at[0, 0],
            recv_sem=tp_recv.at[0, p],
            device_id={"tp": p},
        )

    def wq_sib(p, cc):
        return pltpu.make_async_remote_copy(
            src_ref=wq.at[p, ds(cc * half_feat, half_feat)],
            dst_ref=wq.at[p, ds(cc * half_feat, half_feat)],
            send_sem=sib_send.at[0, p],
            recv_sem=sib_recv.at[0, p],
            device_id={"blk": sibling},
        )

    def wo_copy(i, p):
        return pltpu.make_async_remote_copy(
            src_ref=wo_hbm.at[ds(core * half_width, half_width, 64), ds(p * feat, feat)],
            dst_ref=wo.at[t, ds(core * half_width, half_width, 64)],
            send_sem=tp_send.at[1, i],
            recv_sem=tp_recv.at[1, t],
            device_id={"tp": p},
        )

    def wo_landed(p):
        return pltpu.make_async_remote_copy(
            src_ref=wo.at[p, ds(core * half_width, half_width, 64)],
            dst_ref=wo.at[p, ds(core * half_width, half_width, 64)],
            send_sem=tp_send.at[1, 0],
            recv_sem=tp_recv.at[1, p],
            device_id={"tp": p},
        )

    def wo_sib(p, cc):
        return pltpu.make_async_remote_copy(
            src_ref=wo.at[p, ds(cc * half_width, half_width, 64)],
            dst_ref=wo.at[p, ds(cc * half_width, half_width, 64)],
            send_sem=sib_send.at[1, p],
            recv_sem=sib_recv.at[1, p],
            device_id={"blk": sibling},
        )

    def sq_copy(i, p, slot):
        return pltpu.make_async_remote_copy(
            src_ref=sqbuf.at[slot],
            dst_ref=sqbuf.at[slot],
            send_sem=tp_send.at[2, i],
            recv_sem=tp_recv.at[2, slot],
            device_id={"tp": p},
        )

    def q_copy(i, p, slot):
        return pltpu.make_async_remote_copy(
            src_ref=qsend.at[p],
            dst_ref=qrecv.at[slot],
            send_sem=tp_send.at[3, i],
            recv_sem=tp_recv.at[3, slot],
            device_id={"tp": p},
        )

    def att_copy(i, p, slot):
        return pltpu.make_async_remote_copy(
            src_ref=attbuf.at[slot],
            dst_ref=attbuf.at[slot],
            send_sem=tp_send.at[4, i],
            recv_sem=tp_recv.at[4, slot],
            device_id={"tp": p},
        )

    for i, p in enumerate(peers):
        wq_copy(i, p).start()
    for kv in (0, 1):
        loads[kv].wait()

        @pl.when(has_left)
        def _():
            left_copy(kv, line).start()

        @pl.when(has_right)
        def _():
            right_copy(kv, line).start()

        beside_copy(kv, line).start()
        sib_copy(kv, line).start()

    loads[2].wait()
    tile = column_tile(feat)
    squares = jnp.zeros((rows, 1), jnp.float32)
    for start in range(0, feat, tile):
        piece = xbuf[:, start : start + tile].astype(jnp.float32)
        squares += jnp.sum(piece * piece, axis=1, keepdims=True)
        gain = gain_ref[:, ds(t * feat + start, tile)]
        xg[:, start : start + tile] = (piece * gain).astype(jnp.bfloat16)
    wide = jnp.broadcast_to(squares, (rows, LANES))
    sqbuf[t] = jnp.transpose(wide)[0:8, :]
    loads[3].wait()
    own_part[...] = jnp.dot(xg[...], wq[t], preferred_element_type=jnp.float32)
    for i, p in enumerate(peers):
        sq_copy(i, p, t).start()
    row_max[...] = jnp.full(row_max.shape, -1e30, jnp.float32)
    row_sum[...] = jnp.zeros(row_sum.shape, jnp.float32)
    acc[...] = jnp.zeros(acc.shape, jnp.float32)

    column_event(0, 1)
    column_event(1, 1)
    beside_event(0)
    column_event(0, 2)

    for p in peers:
        wq_landed(p).wait_recv()
        wq_sib(p, core).start()
    for i, p in enumerate(peers):
        wq_sib(p, 1 - core).wait_recv()
        qsend[p] = jnp.dot(xg[...], wq[p], preferred_element_type=jnp.float32).astype(
            jnp.bfloat16
        )
        q_copy(i, p, t).start()
    for i, p in enumerate(peers):
        wo_copy(i, p).start()

    column_event(1, 2)

    total = sqbuf[t][0:1, :]
    for i, p in enumerate(peers):
        sq_copy(i, p, p).wait_recv()
        total = total + sqbuf[p][0:1, :]
    column = jnp.transpose(jnp.broadcast_to(total, (LANES, rows)))
    scale = math.log2(math.e) / math.sqrt(HEAD_DIM)
    factor = lax.rsqrt(column / (feat * n_tp) + NORM_EPS) * scale
    for i, p in enumerate(peers):
        q_copy(i, p, p).wait_recv()
    for h in range(heads):
        cols = slice(h * HEAD_DIM, (h + 1) * HEAD_DIM)
        summed = own_part[:, cols]
        for p in peers:
            summed = summed + qrecv[p, :, cols].astype(jnp.float32)
        qbuf[:, cols] = (summed * factor).astype(jnp.bfloat16)

    def attend(zz, yy):
        for kv in (0, 1):
            wait_slot(kv, zz, yy, 1 - core)
        first = index(zz, yy, 0)

        def one_head(h, carry):
            cols = ds(h * HEAD_DIM, HEAD_DIM)
            keys = kbuf[pl.ds(first, 2), :, cols].reshape(-1, HEAD_DIM)
            vals = vbuf[pl.ds(first, 2), :, cols].reshape(-1, HEAD_DIM)
            scores = lax.dot_general(
                qbuf[:, cols], keys, (((1,), (1,)), ((), ())), preferred_element_type=jnp.float32
            )
            old = row_max[h]
            new = jnp.maximum(old, jnp.max(scores, axis=1, keepdims=True))
            weights = jnp.exp2(scores - new[:, 0:1])
            keep = jnp.exp2(old - new)
            row_max[h] = new
            row_sum[h] = row_sum[h] * keep + jnp.sum(weights, axis=1, keepdims=True)
            mixed = jnp.dot(weights.astype(jnp.bfloat16), vals, preferred_element_type=jnp.float32)
            acc[:, cols] = acc[:, cols] * keep + mixed
            return carry

        lax.fori_loop(0, heads, one_head, 0)

    attend(line, side)
    beside_event(1)
    attend(line, 1 - side)
    attend(nearest(1), side)
    for d in range(2, n_line):
        column_event(0, d + 1)
        attend(nearest(d - 1), 1 - side)
        attend(nearest(d), side)
        column_event(1, d + 1)
        beside_event(d)
    for p in peers:
        wo_landed(p).wait_recv()
        wo_sib(p, core).start()
    attend(nearest(n_line - 1), 1 - side)

    for h in range(heads):
        cols = slice(h * HEAD_DIM, (h + 1) * HEAD_DIM)
        attbuf[t, :, cols] = (acc[:, cols] / row_sum[h]).astype(jnp.bfloat16)
    loads[4].wait()
    for p in peers:
        wo_sib(p, 1 - core).wait_recv()
    for i, p in enumerate(peers):
        att_copy(i, p, t).start()
    for i, p in enumerate(peers):
        att_copy(i, p, p).wait_recv()
    stores = []
    for j, start in enumerate(range(0, feat, tile)):
        cols = slice(start, start + tile)
        result = jnp.zeros((rows, tile), jnp.float32)
        for p in range(n_tp):
            result += jnp.dot(attbuf[p], wo[p, :, cols], preferred_element_type=jnp.float32)
        obuf[:, cols] = result.astype(jnp.bfloat16)
        store = pltpu.make_async_copy(obuf.at[:, cols], out_hbm.at[:, cols], out_sem.at[j])
        store.start()
        stores.append(store)

    for kv in (0, 1):
        for zz in range(n_line):

            @pl.when(has_right & (line >= zz))
            def _():
                right_copy(kv, zz).wait_send()

            @pl.when(has_left & (line <= zz))
            def _():
                left_copy(kv, zz).wait_send()

            beside_copy(kv, zz).wait_send()
            sib_copy(kv, zz).wait_send()
            sib_beside_copy(kv, zz).wait_send()
    for i, p in enumerate(peers):
        wq_copy(i, p).wait_send()
        wo_copy(i, p).wait_send()
        sq_copy(i, p, t).wait_send()
        q_copy(i, p, t).wait_send()
        att_copy(i, p, t).wait_send()
        wq_sib(p, core).wait_send()
        wo_sib(p, core).wait_send()
    for store in stores:
        store.wait()


def per_device(n_blk, n_tp, dec_states, norm_gain, query_weight, out_weight, enc_keys, enc_values):
    rows, feat = dec_states.shape
    width = query_weight.shape[1]
    enc_rows = enc_keys.shape[0]
    heads = width // HEAD_DIM
    n_line = n_blk // 4
    tiles = feat // column_tile(feat)
    bf16, f32 = jnp.bfloat16, jnp.float32
    anywhere = pl.BlockSpec(memory_space=pl.ANY)
    return pl.pallas_call(
        functools.partial(kernel, n_blk, n_tp),
        out_shape=jax.ShapeDtypeStruct((rows, feat), bf16),
        in_specs=[
            anywhere,
            pl.BlockSpec(memory_space=pltpu.VMEM),
            anywhere,
            anywhere,
            anywhere,
            anywhere,
        ],
        out_specs=anywhere,
        scratch_shapes=[
            pltpu.VMEM((n_blk, enc_rows, width), bf16),
            pltpu.VMEM((n_blk, enc_rows, width), bf16),
            pltpu.VMEM((n_tp, feat, width), bf16),
            pltpu.VMEM((n_tp, width, feat), bf16),
            pltpu.VMEM((rows, feat), bf16),
            pltpu.VMEM((rows, feat), bf16),
            pltpu.VMEM((n_tp, rows, width), bf16),
            pltpu.VMEM((n_tp, rows, width), bf16),
            pltpu.VMEM((rows, width), f32),
            pltpu.VMEM((n_tp, 8, rows), f32),
            pltpu.VMEM((rows, width), bf16),
            pltpu.VMEM((n_tp, rows, width), bf16),
            pltpu.VMEM((rows, feat), bf16),
            pltpu.VMEM((heads, rows, LANES), f32),
            pltpu.VMEM((heads, rows, LANES), f32),
            pltpu.VMEM((rows, width), f32),
            pltpu.SemaphoreType.DMA((2, 5, n_line)),
            pltpu.SemaphoreType.DMA((2, n_blk)),
            pltpu.SemaphoreType.DMA((5, n_tp)),
            pltpu.SemaphoreType.DMA((5, n_tp)),
            pltpu.SemaphoreType.DMA((2, n_tp)),
            pltpu.SemaphoreType.DMA((2, n_tp)),
            pltpu.SemaphoreType.DMA((5,)),
            pltpu.SemaphoreType.DMA((tiles,)),
        ],
        compiler_params=pltpu.CompilerParams(
            collective_id=0, has_side_effects=True, vmem_limit_bytes=60 * 1024 * 1024
        ),
    )(dec_states, norm_gain.reshape(1, -1), query_weight, out_weight, enc_keys, enc_values)


def solution(mesh):
    in_specs = (P("blk", "tp"), P(), P(None, "tp"), P("tp", None), P("blk", "tp"), P("blk", "tp"))
    out_specs = P("blk", "tp")
    body = functools.partial(per_device, mesh.shape["blk"], mesh.shape["tp"])
    return jax.shard_map(body, mesh=mesh, in_specs=in_specs, out_specs=out_specs, check_vma=False)
```

```python
import functools
import math

import jax
import jax.numpy as jnp
from jax import lax
from jax.experimental import pallas as pl
from jax.experimental.pallas import tpu as pltpu
from jax.sharding import PartitionSpec as P

HEAD_DIM = 128
NORM_EPS = 1e-06
LANES = 128


def column_tile(width, limit=640):
    best = LANES
    for tile in range(LANES, limit + 1, LANES):
        if width % tile == 0:
            best = tile
    return best


def kernel(
    n_blk,
    n_tp,
    x_hbm,
    gain_ref,
    wq_hbm,
    wo_hbm,
    k_hbm,
    v_hbm,
    out_hbm,
    kvbuf,
    wq,
    wo,
    xbuf,
    xg,
    qsend,
    qrecv,
    own_part,
    sqbuf,
    qbuf,
    attbuf,
    oacc,
    obuf,
    kv_send,
    kv_recv,
    move_send,
    tp_send,
    tp_recv,
    head_send,
    head_recv,
    sib_send,
    sib_recv,
    kv_local,
    wo_local,
    local_sem,
    out_sem,
):
    n_line = n_blk // 4
    b = lax.axis_index("blk")
    t = lax.axis_index("tp")
    core = lax.rem(b, 2)
    side = lax.rem(lax.div(b, 2), 2)
    line = lax.div(b, 4)
    rows = x_hbm.shape[0]
    feat = x_hbm.shape[1]
    width = wq_hbm.shape[1]
    heads = width // HEAD_DIM
    pieces = 2 * heads
    half_feat = feat // 2
    half_head = HEAD_DIM // 2
    moved = tuple(range(1, 1 + pieces // 2))
    ahead = 3

    def index(zz, yy, cc):
        return (zz * 2 + yy) * 2 + cc

    sibling = index(line, side, 1 - core)
    beside = index(line, 1 - side, core)
    peers = [lax.rem(t + off, n_tp) for off in range(1, n_tp)]

    def ds(start, size, mult=LANES):
        return pl.ds(pl.multiple_of(start, mult), size)

    def head_cols(h):
        return slice(h * HEAD_DIM, (h + 1) * HEAD_DIM)

    kv_loads = [
        pltpu.make_async_copy(
            (k_hbm, v_hbm)[e % 2].at[:, head_cols(e // 2)], kvbuf.at[e, b], kv_local.at[e]
        )
        for e in range(pieces)
    ]
    wo_loads = [
        pltpu.make_async_copy(
            wo_hbm.at[head_cols(h), ds(t * feat, feat)], wo.at[t, h], wo_local.at[h]
        )
        for h in range(heads)
    ]
    x_load = pltpu.make_async_copy(x_hbm, xbuf, local_sem.at[0])
    wq_load = pltpu.make_async_copy(wq_hbm.at[ds(t * feat, feat)], wq.at[t], local_sem.at[1])
    for load in kv_loads + [x_load, wq_load] + wo_loads:
        load.start()

    barrier = pltpu.get_barrier_semaphore()
    has_left = line > 0
    has_right = line < n_line - 1

    @pl.when(has_left)
    def _():
        pl.semaphore_signal(barrier, inc=1, device_id={"blk": b - 4})

    @pl.when(has_right)
    def _():
        pl.semaphore_signal(barrier, inc=1, device_id={"blk": b + 4})

    pl.semaphore_signal(barrier, inc=1, device_id={"blk": sibling})
    pl.semaphore_signal(barrier, inc=1, device_id={"blk": beside})
    for p in peers:
        pl.semaphore_signal(barrier, inc=1, device_id={"tp": p})
    ends = jnp.where(has_left, 1, 0) + jnp.where(has_right, 1, 0)
    pl.semaphore_wait(barrier, 2 + len(peers) + ends)

    def kv_copy(e, send_sem, slot, target):
        return pltpu.make_async_remote_copy(
            src_ref=kvbuf.at[e, slot],
            dst_ref=kvbuf.at[e, slot],
            send_sem=send_sem,
            recv_sem=kv_recv.at[e, slot],
            device_id={"blk": target},
        )

    def right_copy(e, zz):
        return kv_copy(e, kv_send.at[e, 0, zz], index(zz, side, core), b + 4)

    def left_copy(e, zz):
        return kv_copy(e, kv_send.at[e, 1, zz], index(zz, side, core), b - 4)

    def beside_copy(e, zz):
        return kv_copy(e, kv_send.at[e, 2, zz], index(zz, side, core), beside)

    def sib_copy(e, zz):
        return kv_copy(e, kv_send.at[e, 3, zz], index(zz, side, core), sibling)

    def sib_beside_copy(e, zz):
        return kv_copy(e, kv_send.at[e, 4, zz], index(zz, 1 - side, core), sibling)

    def move_left(e):
        return kv_copy(e, move_send.at[0, e], index(n_line - 1, 1 - side, core), b - 4)

    def move_right(e):
        return kv_copy(e, move_send.at[1, e], index(0, 1 - side, core), b + 4)

    def goes_beside(e, zz):
        inner = (zz > 0) & (zz < n_line - 1)
        return inner | (zz == line) if e in moved else zz >= 0

    def wait_slot(e, slot):
        kv_copy(e, kv_send.at[e, 0, 0], slot, sibling).wait_recv()

    def own_event(e):
        if e >= pieces:
            return
        kv_loads[e].wait()

        @pl.when(has_left)
        def _():
            left_copy(e, line).start()

        @pl.when(has_right)
        def _():
            right_copy(e, line).start()

        beside_copy(e, line).start()
        sib_copy(e, line).start()

    def column_event(e, d):
        @pl.when(line + d < n_line)
        def _():
            zz = line + d
            wait_slot(e, index(zz, side, core))

            @pl.when(has_left)
            def _():
                left_copy(e, zz).start()

            @pl.when(goes_beside(e, zz))
            def _():
                beside_copy(e, zz).start()

            sib_copy(e, zz).start()

        @pl.when(line - d >= 0)
        def _():
            zz = line - d
            wait_slot(e, index(zz, side, core))

            @pl.when(has_right)
            def _():
                right_copy(e, zz).start()

            @pl.when(goes_beside(e, zz))
            def _():
                beside_copy(e, zz).start()

            sib_copy(e, zz).start()

    def move_event(e, d):
        @pl.when(line + d == n_line - 1)
        def _():
            zz = line + d
            wait_slot(e, index(zz, 1 - side, core))

            @pl.when(has_left)
            def _():
                move_left(e).start()

            sib_beside_copy(e, zz).start()

        @pl.when(line - d == 0)
        def _():
            zz = line - d
            wait_slot(e, index(zz, 1 - side, core))

            @pl.when(has_right)
            def _():
                move_right(e).start()

            sib_beside_copy(e, zz).start()

    def nearest(k):
        short = jnp.minimum(line, n_line - 1 - line)
        swing = line + (k + 1) // 2 if k % 2 == 1 else line - k // 2
        tail = jnp.where(line < n_line - 1 - line, k, n_line - 1 - k)
        return jnp.where(k <= 2 * short, swing, tail)

    def beside_event(e, k):
        zz = nearest(k)

        def handle():
            wait_slot(e, index(zz, 1 - side, core))
            sib_beside_copy(e, zz).start()

        if e in moved:
            pl.when((zz > 0) & (zz < n_line - 1))(handle)
        else:
            handle()

    def wave(s):
        for d in range(1, n_line):
            e = s + 1 - d
            if 0 <= e < pieces:
                column_event(e, d)
        own_event(s + ahead)
        for d in range(n_line):
            if s - d in moved:
                move_event(s - d, d)

    n_waves = pieces + n_line - 2

    def tp_copy(src, dst, send_sem, recv_sem, p):
        return pltpu.make_async_remote_copy(
            src_ref=src, dst_ref=dst, send_sem=send_sem, recv_sem=recv_sem, device_id={"tp": p}
        )

    def wq_half(p, cc):
        return wq.at[p, ds(cc * half_feat, half_feat)]

    def wq_copy(i, p):
        src = wq_hbm.at[ds(p * feat + core * half_feat, half_feat)]
        return tp_copy(src, wq_half(t, core), tp_send.at[0, i], tp_recv.at[0, t], p)

    def wq_landed(p):
        ref = wq_half(p, core)
        return tp_copy(ref, ref, tp_send.at[0, 0], tp_recv.at[0, p], p)

    def wq_sib(p, cc):
        return pltpu.make_async_remote_copy(
            src_ref=wq_half(p, cc),
            dst_ref=wq_half(p, cc),
            send_sem=sib_send.at[heads, p],
            recv_sem=sib_recv.at[heads, p],
            device_id={"blk": sibling},
        )

    def wo_half(p, h, cc):
        return wo.at[p, h, ds(cc * half_head, half_head, half_head)]

    def wo_copy(i, p, h):
        src = wo_hbm.at[ds(h * HEAD_DIM + core * half_head, half_head, half_head), ds(p * feat, feat)]
        return tp_copy(src, wo_half(t, h, core), head_send.at[0, h, i], head_recv.at[0, h, t], p)

    def wo_landed(p, h):
        ref = wo_half(p, h, core)
        return tp_copy(ref, ref, head_send.at[0, h, 0], head_recv.at[0, h, p], p)

    def wo_sib(p, h, cc):
        return pltpu.make_async_remote_copy(
            src_ref=wo_half(p, h, cc),
            dst_ref=wo_half(p, h, cc),
            send_sem=sib_send.at[h, p],
            recv_sem=sib_recv.at[h, p],
            device_id={"blk": sibling},
        )

    def sq_copy(i, p, slot):
        ref = sqbuf.at[slot]
        return tp_copy(ref, ref, tp_send.at[1, i], tp_recv.at[1, slot], p)

    def q_copy(i, p, slot):
        return tp_copy(qsend.at[p], qrecv.at[slot], tp_send.at[2, i], tp_recv.at[2, slot], p)

    def att_copy(i, p, h, slot):
        ref = attbuf.at[slot, h]
        return tp_copy(ref, ref, head_send.at[1, h, i], head_recv.at[1, h, slot], p)

    for i, p in enumerate(peers):
        wq_copy(i, p).start()
    for e in range(ahead):
        own_event(e)

    x_load.wait()
    tile = column_tile(feat)
    squares = jnp.zeros((rows, 1), jnp.float32)
    for start in range(0, feat, tile):
        piece = xbuf[:, start : start + tile].astype(jnp.float32)
        squares += jnp.sum(piece * piece, axis=1, keepdims=True)
        gain = gain_ref[:, ds(t * feat + start, tile)]
        xg[:, start : start + tile] = (piece * gain).astype(jnp.bfloat16)
    wide = jnp.broadcast_to(squares, (rows, LANES))
    sqbuf[t] = jnp.transpose(wide)[0:8, :]
    wave(0)
    wq_load.wait()
    own_part[...] = jnp.dot(xg[...], wq[t], preferred_element_type=jnp.float32)
    for i, p in enumerate(peers):
        sq_copy(i, p, t).start()
    weights_wave = n_waves // 2
    for s in range(1, weights_wave):
        wave(s)

    for p in peers:
        wq_landed(p).wait_recv()
        wq_sib(p, core).start()
    for i, p in enumerate(peers):
        wq_sib(p, 1 - core).wait_recv()
        qsend[p] = jnp.dot(xg[...], wq[p], preferred_element_type=jnp.float32).astype(
            jnp.bfloat16
        )
        q_copy(i, p, t).start()
    for h in range(heads - 1):
        for i, p in enumerate(peers):
            wo_copy(i, p, h).start()

    wave(weights_wave)

    total = sqbuf[t][0:1, :]
    for i, p in enumerate(peers):
        sq_copy(i, p, p).wait_recv()
        total = total + sqbuf[p][0:1, :]
    column = jnp.transpose(jnp.broadcast_to(total, (LANES, rows)))
    scale = math.log2(math.e) / math.sqrt(HEAD_DIM)
    factor = lax.rsqrt(column / (feat * n_tp) + NORM_EPS) * scale
    for i, p in enumerate(peers):
        q_copy(i, p, p).wait_recv()
    for h in range(heads):
        summed = own_part[:, head_cols(h)]
        for p in peers:
            summed = summed + qrecv[p, :, head_cols(h)].astype(jnp.float32)
        qbuf[:, head_cols(h)] = (summed * factor).astype(jnp.bfloat16)

    def attend(h, state, zz, yy):
        for e in (2 * h, 2 * h + 1):
            wait_slot(e, index(zz, yy, 1 - core))
        first = index(zz, yy, 0)
        keys = kvbuf[2 * h, pl.ds(first, 2)].reshape(-1, HEAD_DIM)
        vals = kvbuf[2 * h + 1, pl.ds(first, 2)].reshape(-1, HEAD_DIM)
        scores = lax.dot_general(
            qbuf[:, head_cols(h)],
            keys,
            (((1,), (1,)), ((), ())),
            preferred_element_type=jnp.float32,
        )
        old, row_sum, acc = state
        new = jnp.maximum(old, jnp.max(scores, axis=1, keepdims=True))
        weights = jnp.exp2(scores - new)
        keep = jnp.exp2(old - new)
        row_sum = row_sum * keep + jnp.sum(weights, axis=1, keepdims=True)
        mixed = jnp.dot(weights.astype(jnp.bfloat16), vals, preferred_element_type=jnp.float32)
        return new, row_sum, acc * keep + mixed

    def head_attention(h):
        state = (
            jnp.full((rows, 1), -1e30, jnp.float32),
            jnp.zeros((rows, 1), jnp.float32),
            jnp.zeros((rows, HEAD_DIM), jnp.float32),
        )
        for e in (2 * h, 2 * h + 1):
            beside_event(e, 0)
        for k in range(n_line):
            state = attend(h, state, nearest(k), side)
            if k >= 1:
                state = attend(h, state, nearest(k - 1), 1 - side)
            if k + 1 < n_line:
                for e in (2 * h, 2 * h + 1):
                    beside_event(e, k + 1)
        unused, row_sum, acc = attend(h, state, nearest(n_line - 1), 1 - side)
        attbuf[t, h] = (acc / row_sum).astype(jnp.bfloat16)
        for i, p in enumerate(peers):
            att_copy(i, p, h, t).start()

    done = weights_wave + 1
    for h in range(heads):
        need = n_waves if h == heads - 1 else min(2 * h + 1 + n_line, n_waves)
        while done < need:
            wave(done)
            done += 1
        for hh in range(heads - 1):
            if h == heads - 1:
                for p in peers:
                    wo_landed(p, hh).wait_recv()
                    wo_sib(p, hh, core).start()
        head_attention(h)
        if h == 0:
            for i, p in enumerate(peers):
                wo_copy(i, p, heads - 1).start()

    last = heads - 1
    for p in peers:
        wo_landed(p, last).wait_recv()
        wo_sib(p, last, core).start()
    for load in wo_loads:
        load.wait()
    for h in range(heads - 1):
        for i, p in enumerate(peers):
            wo_sib(p, h, 1 - core).wait_recv()
            att_copy(i, p, h, p).wait_recv()
    starts = range(0, feat, tile)
    for start in starts:
        cols = slice(start, start + tile)
        result = jnp.dot(attbuf[t, last], wo[t, last, :, cols], preferred_element_type=jnp.float32)
        for p in range(n_tp):
            for h in range(heads - 1):
                result += jnp.dot(
                    attbuf[p, h], wo[p, h, :, cols], preferred_element_type=jnp.float32
                )
        oacc[:, cols] = result
    for i, p in enumerate(peers):
        wo_sib(p, last, 1 - core).wait_recv()
        att_copy(i, p, last, p).wait_recv()
    stores = []
    for j, start in enumerate(starts):
        cols = slice(start, start + tile)
        result = oacc[:, cols]
        for p in peers:
            result += jnp.dot(
                attbuf[p, last], wo[p, last, :, cols], preferred_element_type=jnp.float32
            )
        obuf[:, cols] = result.astype(jnp.bfloat16)
        store = pltpu.make_async_copy(obuf.at[:, cols], out_hbm.at[:, cols], out_sem.at[j])
        store.start()
        stores.append(store)

    for e in range(pieces):
        for zz in range(n_line):

            @pl.when(has_right & (line >= zz))
            def _():
                right_copy(e, zz).wait_send()

            @pl.when(has_left & (line <= zz))
            def _():
                left_copy(e, zz).wait_send()

            if e in moved and zz in (0, n_line - 1):

                @pl.when(line == zz)
                def _():
                    beside_copy(e, zz).wait_send()

            else:
                beside_copy(e, zz).wait_send()
            sib_copy(e, zz).wait_send()
            sib_beside_copy(e, zz).wait_send()
        if e in moved:

            @pl.when(has_left)
            def _():
                move_left(e).wait_send()

            @pl.when(has_right)
            def _():
                move_right(e).wait_send()

    for i, p in enumerate(peers):
        wq_copy(i, p).wait_send()
        sq_copy(i, p, t).wait_send()
        q_copy(i, p, t).wait_send()
        wq_sib(p, core).wait_send()
        for h in range(heads):
            wo_copy(i, p, h).wait_send()
            att_copy(i, p, h, t).wait_send()
            wo_sib(p, h, core).wait_send()
    for store in stores:
        store.wait()


def per_device(n_blk, n_tp, dec_states, norm_gain, query_weight, out_weight, enc_keys, enc_values):
    rows, feat = dec_states.shape
    width = query_weight.shape[1]
    enc_rows = enc_keys.shape[0]
    heads = width // HEAD_DIM
    n_line = n_blk // 4
    tiles = feat // column_tile(feat)
    bf16, f32 = jnp.bfloat16, jnp.float32
    dma = pltpu.SemaphoreType.DMA
    anywhere = pl.BlockSpec(memory_space=pl.ANY)
    return pl.pallas_call(
        functools.partial(kernel, n_blk, n_tp),
        out_shape=jax.ShapeDtypeStruct((rows, feat), bf16),
        in_specs=[
            anywhere,
            pl.BlockSpec(memory_space=pltpu.VMEM),
            anywhere,
            anywhere,
            anywhere,
            anywhere,
        ],
        out_specs=anywhere,
        scratch_shapes=[
            pltpu.VMEM((2 * heads, n_blk, enc_rows, HEAD_DIM), bf16),
            pltpu.VMEM((n_tp, feat, width), bf16),
            pltpu.VMEM((n_tp, heads, HEAD_DIM, feat), bf16),
            pltpu.VMEM((rows, feat), bf16),
            pltpu.VMEM((rows, feat), bf16),
            pltpu.VMEM((n_tp, rows, width), bf16),
            pltpu.VMEM((n_tp, rows, width), bf16),
            pltpu.VMEM((rows, width), f32),
            pltpu.VMEM((n_tp, 8, rows), f32),
            pltpu.VMEM((rows, width), bf16),
            pltpu.VMEM((n_tp, heads, rows, HEAD_DIM), bf16),
            pltpu.VMEM((rows, feat), f32),
            pltpu.VMEM((rows, feat), bf16),
            dma((2 * heads, 5, n_line)),
            dma((2 * heads, n_blk)),
            dma((2, 2 * heads)),
            dma((3, n_tp)),
            dma((3, n_tp)),
            dma((2, heads, n_tp)),
            dma((2, heads, n_tp)),
            dma((heads + 1, n_tp)),
            dma((heads + 1, n_tp)),
            dma((2 * heads,)),
            dma((heads,)),
            dma((2,)),
            dma((tiles,)),
        ],
        compiler_params=pltpu.CompilerParams(
            collective_id=0, has_side_effects=True, vmem_limit_bytes=60 * 1024 * 1024
        ),
    )(dec_states, norm_gain.reshape(1, -1), query_weight, out_weight, enc_keys, enc_values)


def solution(mesh):
    in_specs = (P("blk", "tp"), P(), P(None, "tp"), P("tp", None), P("blk", "tp"), P("blk", "tp"))
    out_specs = P("blk", "tp")
    body = functools.partial(per_device, mesh.shape["blk"], mesh.shape["tp"])
    return jax.shard_map(body, mesh=mesh, in_specs=in_specs, out_specs=out_specs, check_vma=False)
```

```python
import functools
import math

import jax
import jax.numpy as jnp
from jax import lax
from jax.experimental import pallas as pl
from jax.experimental.pallas import tpu as pltpu
from jax.sharding import PartitionSpec as P

HEAD_DIM = 128
NORM_EPS = 1e-06
LANES = 128


def column_tile(width, limit=640):
    best = LANES
    for tile in range(LANES, limit + 1, LANES):
        if width % tile == 0:
            best = tile
    return best


def kernel(
    n_blk,
    n_tp,
    x_hbm,
    gain_ref,
    wq_hbm,
    wo_hbm,
    k_hbm,
    v_hbm,
    out_hbm,
    kvbuf,
    wq,
    wo,
    xbuf,
    xg,
    qsend,
    qrecv,
    own_part,
    sqbuf,
    qbuf,
    attbuf,
    oacc,
    obuf,
    kv_send,
    kv_recv,
    move_send,
    tp_send,
    tp_recv,
    head_send,
    head_recv,
    sib_send,
    sib_recv,
    kv_local,
    wo_local,
    local_sem,
    out_sem,
):
    n_line = n_blk // 4
    b = lax.axis_index("blk")
    t = lax.axis_index("tp")
    core = lax.rem(b, 2)
    side = lax.rem(lax.div(b, 2), 2)
    line = lax.div(b, 4)
    rows = x_hbm.shape[0]
    feat = x_hbm.shape[1]
    width = wq_hbm.shape[1]
    heads = width // HEAD_DIM
    pieces = 2 * heads
    half_feat = feat // 2
    half_head = HEAD_DIM // 2
    moved = ()
    ahead = 3

    def index(zz, yy, cc):
        return (zz * 2 + yy) * 2 + cc

    sibling = index(line, side, 1 - core)
    beside = index(line, 1 - side, core)
    peers = [lax.rem(t + off, n_tp) for off in range(1, n_tp)]

    def ds(start, size, mult=LANES):
        return pl.ds(pl.multiple_of(start, mult), size)

    def head_cols(h):
        return slice(h * HEAD_DIM, (h + 1) * HEAD_DIM)

    kv_loads = [
        pltpu.make_async_copy(
            (k_hbm, v_hbm)[e % 2].at[:, head_cols(e // 2)], kvbuf.at[e, b], kv_local.at[e]
        )
        for e in range(pieces)
    ]
    wo_loads = [
        pltpu.make_async_copy(
            wo_hbm.at[head_cols(h), ds(t * feat, feat)], wo.at[t, h], wo_local.at[h]
        )
        for h in range(heads)
    ]
    x_load = pltpu.make_async_copy(x_hbm, xbuf, local_sem.at[0])
    wq_load = pltpu.make_async_copy(wq_hbm.at[ds(t * feat, feat)], wq.at[t], local_sem.at[1])
    for load in kv_loads + [x_load, wq_load] + wo_loads:
        load.start()

    barrier = pltpu.get_barrier_semaphore()
    has_left = line > 0
    has_right = line < n_line - 1

    @pl.when(has_left)
    def _():
        pl.semaphore_signal(barrier, inc=1, device_id={"blk": b - 4})

    @pl.when(has_right)
    def _():
        pl.semaphore_signal(barrier, inc=1, device_id={"blk": b + 4})

    pl.semaphore_signal(barrier, inc=1, device_id={"blk": sibling})
    pl.semaphore_signal(barrier, inc=1, device_id={"blk": beside})
    for p in peers:
        pl.semaphore_signal(barrier, inc=1, device_id={"tp": p})
    ends = jnp.where(has_left, 1, 0) + jnp.where(has_right, 1, 0)
    pl.semaphore_wait(barrier, 2 + len(peers) + ends)

    def kv_copy(e, send_sem, slot, target):
        return pltpu.make_async_remote_copy(
            src_ref=kvbuf.at[e, slot],
            dst_ref=kvbuf.at[e, slot],
            send_sem=send_sem,
            recv_sem=kv_recv.at[e, slot],
            device_id={"blk": target},
        )

    def right_copy(e, zz):
        return kv_copy(e, kv_send.at[e, 0, zz], index(zz, side, core), b + 4)

    def left_copy(e, zz):
        return kv_copy(e, kv_send.at[e, 1, zz], index(zz, side, core), b - 4)

    def beside_copy(e, zz):
        return kv_copy(e, kv_send.at[e, 2, zz], index(zz, side, core), beside)

    def sib_copy(e, zz):
        return kv_copy(e, kv_send.at[e, 3, zz], index(zz, side, core), sibling)

    def sib_beside_copy(e, zz):
        return kv_copy(e, kv_send.at[e, 4, zz], index(zz, 1 - side, core), sibling)

    def move_left(e):
        return kv_copy(e, move_send.at[0, e], index(n_line - 1, 1 - side, core), b - 4)

    def move_right(e):
        return kv_copy(e, move_send.at[1, e], index(0, 1 - side, core), b + 4)

    def goes_beside(e, zz):
        inner = (zz > 0) & (zz < n_line - 1)
        return inner | (zz == line) if e in moved else zz >= 0

    def wait_slot(e, slot):
        kv_copy(e, kv_send.at[e, 0, 0], slot, sibling).wait_recv()

    def own_event(e):
        if e >= pieces:
            return
        kv_loads[e].wait()

        @pl.when(has_left)
        def _():
            left_copy(e, line).start()

        @pl.when(has_right)
        def _():
            right_copy(e, line).start()

        beside_copy(e, line).start()
        sib_copy(e, line).start()

    def column_event(e, d):
        @pl.when(line + d < n_line)
        def _():
            zz = line + d
            wait_slot(e, index(zz, side, core))

            @pl.when(has_left)
            def _():
                left_copy(e, zz).start()

            @pl.when(goes_beside(e, zz))
            def _():
                beside_copy(e, zz).start()

            sib_copy(e, zz).start()

        @pl.when(line - d >= 0)
        def _():
            zz = line - d
            wait_slot(e, index(zz, side, core))

            @pl.when(has_right)
            def _():
                right_copy(e, zz).start()

            @pl.when(goes_beside(e, zz))
            def _():
                beside_copy(e, zz).start()

            sib_copy(e, zz).start()

    def move_event(e, d):
        @pl.when(line + d == n_line - 1)
        def _():
            zz = line + d
            wait_slot(e, index(zz, 1 - side, core))

            @pl.when(has_left)
            def _():
                move_left(e).start()

            sib_beside_copy(e, zz).start()

        @pl.when(line - d == 0)
        def _():
            zz = line - d
            wait_slot(e, index(zz, 1 - side, core))

            @pl.when(has_right)
            def _():
                move_right(e).start()

            sib_beside_copy(e, zz).start()

    def nearest(k):
        short = jnp.minimum(line, n_line - 1 - line)
        swing = line + (k + 1) // 2 if k % 2 == 1 else line - k // 2
        tail = jnp.where(line < n_line - 1 - line, k, n_line - 1 - k)
        return jnp.where(k <= 2 * short, swing, tail)

    def beside_event(e, k):
        zz = nearest(k)

        def handle():
            wait_slot(e, index(zz, 1 - side, core))
            sib_beside_copy(e, zz).start()

        if e in moved:
            pl.when((zz > 0) & (zz < n_line - 1))(handle)
        else:
            handle()

    def wave(s):
        for d in range(1, n_line):
            e = s + 1 - d
            if 0 <= e < pieces:
                column_event(e, d)
        own_event(s + ahead)
        for d in range(n_line):
            if s - d in moved:
                move_event(s - d, d)

    n_waves = pieces + n_line - 2

    def tp_copy(src, dst, send_sem, recv_sem, p):
        return pltpu.make_async_remote_copy(
            src_ref=src, dst_ref=dst, send_sem=send_sem, recv_sem=recv_sem, device_id={"tp": p}
        )

    def wq_half(p, cc):
        return wq.at[p, ds(cc * half_feat, half_feat)]

    def wq_copy(i, p):
        src = wq_hbm.at[ds(p * feat + core * half_feat, half_feat)]
        return tp_copy(src, wq_half(t, core), tp_send.at[0, i], tp_recv.at[0, t], p)

    def wq_landed(p):
        ref = wq_half(p, core)
        return tp_copy(ref, ref, tp_send.at[0, 0], tp_recv.at[0, p], p)

    def wq_sib(p, cc):
        return pltpu.make_async_remote_copy(
            src_ref=wq_half(p, cc),
            dst_ref=wq_half(p, cc),
            send_sem=sib_send.at[heads, p],
            recv_sem=sib_recv.at[heads, p],
            device_id={"blk": sibling},
        )

    def wo_half(p, h, cc):
        return wo.at[p, h, ds(cc * half_head, half_head, half_head)]

    def wo_copy(i, p, h):
        src = wo_hbm.at[ds(h * HEAD_DIM + core * half_head, half_head, half_head), ds(p * feat, feat)]
        return tp_copy(src, wo_half(t, h, core), head_send.at[0, h, i], head_recv.at[0, h, t], p)

    def wo_landed(p, h):
        ref = wo_half(p, h, core)
        return tp_copy(ref, ref, head_send.at[0, h, 0], head_recv.at[0, h, p], p)

    def wo_sib(p, h, cc):
        return pltpu.make_async_remote_copy(
            src_ref=wo_half(p, h, cc),
            dst_ref=wo_half(p, h, cc),
            send_sem=sib_send.at[h, p],
            recv_sem=sib_recv.at[h, p],
            device_id={"blk": sibling},
        )

    def sq_copy(i, p, slot):
        ref = sqbuf.at[slot]
        return tp_copy(ref, ref, tp_send.at[1, i], tp_recv.at[1, slot], p)

    def q_copy(i, p, slot):
        return tp_copy(qsend.at[p], qrecv.at[slot], tp_send.at[2, i], tp_recv.at[2, slot], p)

    def att_copy(i, p, h, slot):
        ref = attbuf.at[slot, h]
        return tp_copy(ref, ref, head_send.at[1, h, i], head_recv.at[1, h, slot], p)

    for i, p in enumerate(peers):
        wq_copy(i, p).start()
    for e in range(ahead):
        own_event(e)

    x_load.wait()
    tile = column_tile(feat)
    squares = jnp.zeros((rows, 1), jnp.float32)
    for start in range(0, feat, tile):
        piece = xbuf[:, start : start + tile].astype(jnp.float32)
        squares += jnp.sum(piece * piece, axis=1, keepdims=True)
        gain = gain_ref[:, ds(t * feat + start, tile)]
        xg[:, start : start + tile] = (piece * gain).astype(jnp.bfloat16)
    wide = jnp.broadcast_to(squares, (rows, LANES))
    sqbuf[t] = jnp.transpose(wide)[0:8, :]
    wave(0)
    wq_load.wait()
    own_part[...] = jnp.dot(xg[...], wq[t], preferred_element_type=jnp.float32)
    for i, p in enumerate(peers):
        sq_copy(i, p, t).start()
    weights_wave = n_waves // 2
    for s in range(1, weights_wave):
        wave(s)

    for p in peers:
        wq_landed(p).wait_recv()
        wq_sib(p, core).start()
    for i, p in enumerate(peers):
        wq_sib(p, 1 - core).wait_recv()
        qsend[p] = jnp.dot(xg[...], wq[p], preferred_element_type=jnp.float32).astype(
            jnp.bfloat16
        )
        q_copy(i, p, t).start()
    for h in range(heads - 1):
        for i, p in enumerate(peers):
            wo_copy(i, p, h).start()

    wave(weights_wave)

    total = sqbuf[t][0:1, :]
    for i, p in enumerate(peers):
        sq_copy(i, p, p).wait_recv()
        total = total + sqbuf[p][0:1, :]
    column = jnp.transpose(jnp.broadcast_to(total, (LANES, rows)))
    scale = math.log2(math.e) / math.sqrt(HEAD_DIM)
    factor = lax.rsqrt(column / (feat * n_tp) + NORM_EPS) * scale
    for i, p in enumerate(peers):
        q_copy(i, p, p).wait_recv()
    for h in range(heads):
        summed = own_part[:, head_cols(h)]
        for p in peers:
            summed = summed + qrecv[p, :, head_cols(h)].astype(jnp.float32)
        qbuf[:, head_cols(h)] = (summed * factor).astype(jnp.bfloat16)

    def attend(h, state, zz, yy):
        for e in (2 * h, 2 * h + 1):
            wait_slot(e, index(zz, yy, 1 - core))
        first = index(zz, yy, 0)
        keys = kvbuf[2 * h, pl.ds(first, 2)].reshape(-1, HEAD_DIM)
        vals = kvbuf[2 * h + 1, pl.ds(first, 2)].reshape(-1, HEAD_DIM)
        scores = lax.dot_general(
            qbuf[:, head_cols(h)],
            keys,
            (((1,), (1,)), ((), ())),
            preferred_element_type=jnp.float32,
        )
        old, row_sum, acc = state
        new = jnp.maximum(old, jnp.max(scores, axis=1, keepdims=True))
        weights = jnp.exp2(scores - new)
        keep = jnp.exp2(old - new)
        row_sum = row_sum * keep + jnp.sum(weights, axis=1, keepdims=True)
        mixed = jnp.dot(weights.astype(jnp.bfloat16), vals, preferred_element_type=jnp.float32)
        return new, row_sum, acc * keep + mixed

    def head_attention(h):
        state = (
            jnp.full((rows, 1), -1e30, jnp.float32),
            jnp.zeros((rows, 1), jnp.float32),
            jnp.zeros((rows, HEAD_DIM), jnp.float32),
        )
        for e in (2 * h, 2 * h + 1):
            beside_event(e, 0)
        for k in range(n_line):
            state = attend(h, state, nearest(k), side)
            if k >= 1:
                state = attend(h, state, nearest(k - 1), 1 - side)
            if k + 1 < n_line:
                for e in (2 * h, 2 * h + 1):
                    beside_event(e, k + 1)
        unused, row_sum, acc = attend(h, state, nearest(n_line - 1), 1 - side)
        attbuf[t, h] = (acc / row_sum).astype(jnp.bfloat16)
        for i, p in enumerate(peers):
            att_copy(i, p, h, t).start()

    done = weights_wave + 1
    for h in range(heads):
        need = n_waves if h == heads - 1 else min(2 * h + 1 + n_line, n_waves)
        while done < need:
            wave(done)
            done += 1
        for hh in range(heads - 1):
            if h == heads - 1:
                for p in peers:
                    wo_landed(p, hh).wait_recv()
                    wo_sib(p, hh, core).start()
        head_attention(h)
        if h == 0:
            for i, p in enumerate(peers):
                wo_copy(i, p, heads - 1).start()

    last = heads - 1
    for p in peers:
        wo_landed(p, last).wait_recv()
        wo_sib(p, last, core).start()
    for load in wo_loads:
        load.wait()
    for h in range(heads - 1):
        for i, p in enumerate(peers):
            wo_sib(p, h, 1 - core).wait_recv()
            att_copy(i, p, h, p).wait_recv()
    starts = range(0, feat, tile)
    for start in starts:
        cols = slice(start, start + tile)
        result = jnp.dot(attbuf[t, last], wo[t, last, :, cols], preferred_element_type=jnp.float32)
        for p in range(n_tp):
            for h in range(heads - 1):
                result += jnp.dot(
                    attbuf[p, h], wo[p, h, :, cols], preferred_element_type=jnp.float32
                )
        oacc[:, cols] = result
    for i, p in enumerate(peers):
        wo_sib(p, last, 1 - core).wait_recv()
        att_copy(i, p, last, p).wait_recv()
    stores = []
    for j, start in enumerate(starts):
        cols = slice(start, start + tile)
        result = oacc[:, cols]
        for p in peers:
            result += jnp.dot(
                attbuf[p, last], wo[p, last, :, cols], preferred_element_type=jnp.float32
            )
        obuf[:, cols] = result.astype(jnp.bfloat16)
        store = pltpu.make_async_copy(obuf.at[:, cols], out_hbm.at[:, cols], out_sem.at[j])
        store.start()
        stores.append(store)

    for e in range(pieces):
        for zz in range(n_line):

            @pl.when(has_right & (line >= zz))
            def _():
                right_copy(e, zz).wait_send()

            @pl.when(has_left & (line <= zz))
            def _():
                left_copy(e, zz).wait_send()

            if e in moved and zz in (0, n_line - 1):

                @pl.when(line == zz)
                def _():
                    beside_copy(e, zz).wait_send()

            else:
                beside_copy(e, zz).wait_send()
            sib_copy(e, zz).wait_send()
            sib_beside_copy(e, zz).wait_send()
        if e in moved:

            @pl.when(has_left)
            def _():
                move_left(e).wait_send()

            @pl.when(has_right)
            def _():
                move_right(e).wait_send()

    for i, p in enumerate(peers):
        wq_copy(i, p).wait_send()
        sq_copy(i, p, t).wait_send()
        q_copy(i, p, t).wait_send()
        wq_sib(p, core).wait_send()
        for h in range(heads):
            wo_copy(i, p, h).wait_send()
            att_copy(i, p, h, t).wait_send()
            wo_sib(p, h, core).wait_send()
    for store in stores:
        store.wait()


def per_device(n_blk, n_tp, dec_states, norm_gain, query_weight, out_weight, enc_keys, enc_values):
    rows, feat = dec_states.shape
    width = query_weight.shape[1]
    enc_rows = enc_keys.shape[0]
    heads = width // HEAD_DIM
    n_line = n_blk // 4
    tiles = feat // column_tile(feat)
    bf16, f32 = jnp.bfloat16, jnp.float32
    dma = pltpu.SemaphoreType.DMA
    anywhere = pl.BlockSpec(memory_space=pl.ANY)
    return pl.pallas_call(
        functools.partial(kernel, n_blk, n_tp),
        out_shape=jax.ShapeDtypeStruct((rows, feat), bf16),
        in_specs=[
            anywhere,
            pl.BlockSpec(memory_space=pltpu.VMEM),
            anywhere,
            anywhere,
            anywhere,
            anywhere,
        ],
        out_specs=anywhere,
        scratch_shapes=[
            pltpu.VMEM((2 * heads, n_blk, enc_rows, HEAD_DIM), bf16),
            pltpu.VMEM((n_tp, feat, width), bf16),
            pltpu.VMEM((n_tp, heads, HEAD_DIM, feat), bf16),
            pltpu.VMEM((rows, feat), bf16),
            pltpu.VMEM((rows, feat), bf16),
            pltpu.VMEM((n_tp, rows, width), bf16),
            pltpu.VMEM((n_tp, rows, width), bf16),
            pltpu.VMEM((rows, width), f32),
            pltpu.VMEM((n_tp, 8, rows), f32),
            pltpu.VMEM((rows, width), bf16),
            pltpu.VMEM((n_tp, heads, rows, HEAD_DIM), bf16),
            pltpu.VMEM((rows, feat), f32),
            pltpu.VMEM((rows, feat), bf16),
            dma((2 * heads, 5, n_line)),
            dma((2 * heads, n_blk)),
            dma((2, 2 * heads)),
            dma((3, n_tp)),
            dma((3, n_tp)),
            dma((2, heads, n_tp)),
            dma((2, heads, n_tp)),
            dma((heads + 1, n_tp)),
            dma((heads + 1, n_tp)),
            dma((2 * heads,)),
            dma((heads,)),
            dma((2,)),
            dma((tiles,)),
        ],
        compiler_params=pltpu.CompilerParams(
            collective_id=0, has_side_effects=True, vmem_limit_bytes=60 * 1024 * 1024
        ),
    )(dec_states, norm_gain.reshape(1, -1), query_weight, out_weight, enc_keys, enc_values)


def solution(mesh):
    in_specs = (P("blk", "tp"), P(), P(None, "tp"), P("tp", None), P("blk", "tp"), P("blk", "tp"))
    out_specs = P("blk", "tp")
    body = functools.partial(per_device, mesh.shape["blk"], mesh.shape["tp"])
    return jax.shard_map(body, mesh=mesh, in_specs=in_specs, out_specs=out_specs, check_vma=False)
```
